8 devices in a mesh: dp: 2 (over z, y), sp: 4 (over x, core).
Axes of the slice: x: 2, y: 2, z: 1, core: 2. Of those that a mesh axis runs over, the one named last changes fastest.
Arguments:
- act_in: bfloat16 [2, 1024, 2048], P('dp', 'sp')
- positions: int32 [2, 1024], P('dp', 'sp')
- out_grad: bfloat16 [2, 1024, 2048], P('dp', 'sp')
- norm1_gain: bfloat16 [2048], P(('dp', 'sp'))
- norm2_gain: bfloat16 [2048], P(('dp', 'sp'))
- w_query: bfloat16 [2048, 32, 64], P(('dp', 'sp'))
- w_key: bfloat16 [2048, 32, 64], P(('dp', 'sp'))
- w_value: bfloat16 [2048, 32, 64], P(('dp', 'sp'))
- w_out: bfloat16 [2048, 2048], P(('dp', 'sp'))
- w_gate: bfloat16 [2048, 8192], P(('dp', 'sp'))
- w_up: bfloat16 [2048, 8192], P(('dp', 'sp'))
- w_down: bfloat16 [8192, 2048], P(('dp', 'sp'))
Outputs:
- output 1: bfloat16 [2, 1024, 2048], P('dp', 'sp')
- output 2: bfloat16 [2, 1024, 2048], P('dp', 'sp')
- output 3: float32 [2048], P(('dp', 'sp'))
- output 4: float32 [2048], P(('dp', 'sp'))
- output 5: float32 [2048, 32, 64], P(('dp', 'sp'))
- output 6: float32 [2048, 32, 64], P(('dp', 'sp'))
- output 7: float32 [2048, 32, 64], P(('dp', 'sp'))
- output 8: float32 [2048, 2048], P(('dp', 'sp'))
- output 9: float32 [2048, 8192], P(('dp', 'sp'))
- output 10: float32 [2048, 8192], P(('dp', 'sp'))
- output 11: float32 [8192, 2048], P(('dp', 'sp'))
All inputs are finite; a program needn't handle non-finite values.
Results may differ from the reference program's by a relative error of at most 0.0161443.
Values are sent between devices in bfloat16 or wider.
A program may use at most 1 GiB of HBM per device.

```python
import math
import jax
import jax.numpy as jnp
from jax import lax

MODEL_DIM = 2048
Q_HEADS = 32
KV_HEADS = 32
HEAD_DIM = 64
FFN_DIM = 8192
TOKENS_DEV = 256
DP_SIZE = 2
SP_SIZE = 4

SEQ_LEN = TOKENS_DEV * SP_SIZE
HALF_DIM = HEAD_DIM // 2
N_GROUP = Q_HEADS // KV_HEADS
Q_BLOCK = math.gcd(SEQ_LEN, 256)
N_BLOCKS = SEQ_LEN // Q_BLOCK
ATTN_SCALE = HEAD_DIM ** -0.5
EPS = 1e-5
ROPE_BASE = 10000.0
QK_GAIN = 1.5
NEG_BIG = -1e30


def draw_weight(draw_key, shape, fan_in, gain_factor):
    return (jax.random.normal(draw_key, shape, jnp.float32) * (gain_factor * fan_in ** -0.5)).astype(jnp.bfloat16)


def setup_inputs(seed: int = 0) -> dict:
    key_list = jax.random.split(jax.random.key(seed), 12)
    row_shape = (DP_SIZE, SEQ_LEN, MODEL_DIM)
    q_width = Q_HEADS * HEAD_DIM
    pos_steps = jax.random.randint(key_list[1], (DP_SIZE, SEQ_LEN), 1, 3)
    return dict(
        act_in=jax.random.normal(key_list[0], row_shape, jnp.float32).astype(jnp.bfloat16),
        positions=(jnp.cumsum(pos_steps, axis=1) - 1).astype(jnp.int32),
        out_grad=jax.random.normal(key_list[2], row_shape, jnp.float32).astype(jnp.bfloat16),
        norm1_gain=jax.random.uniform(key_list[3], (MODEL_DIM,), jnp.float32, 0.5, 1.5).astype(jnp.bfloat16),
        norm2_gain=jax.random.uniform(key_list[4], (MODEL_DIM,), jnp.float32, 0.5, 1.5).astype(jnp.bfloat16),
        w_query=draw_weight(key_list[5], (MODEL_DIM, Q_HEADS, HEAD_DIM), MODEL_DIM, QK_GAIN),
        w_key=draw_weight(key_list[6], (MODEL_DIM, KV_HEADS, HEAD_DIM), MODEL_DIM, QK_GAIN),
        w_value=draw_weight(key_list[7], (MODEL_DIM, KV_HEADS, HEAD_DIM), MODEL_DIM, 1.0),
        w_out=draw_weight(key_list[8], (q_width, MODEL_DIM), q_width, 1.0),
        w_gate=draw_weight(key_list[9], (MODEL_DIM, FFN_DIM), MODEL_DIM, 1.0),
        w_up=draw_weight(key_list[10], (MODEL_DIM, FFN_DIM), MODEL_DIM, 1.0),
        w_down=draw_weight(key_list[11], (FFN_DIM, MODEL_DIM), FFN_DIM, 1.0),
    )


def rms_scale(rows_f32):
    return lax.rsqrt(jnp.mean(rows_f32 * rows_f32, axis=-1, keepdims=True) + EPS)


def to_bf(values):
    return values.astype(jnp.bfloat16).astype(jnp.float32)


def rope_apply(values, positions):
    inv_freq = ROPE_BASE ** (-(jnp.arange(HALF_DIM, dtype=jnp.float32) * (2.0 / HEAD_DIM)))
    angles = positions.astype(jnp.float32)[:, None] * inv_freq[None, :]
    cos_t = jnp.cos(angles)[:, None, :]
    sin_t = jnp.sin(angles)[:, None, :]
    first_half = values[..., :HALF_DIM]
    second_half = values[..., HALF_DIM:]
    return jnp.concatenate([first_half * cos_t - second_half * sin_t, second_half * cos_t + first_half * sin_t], axis=-1)


def layer_forward(weights, act_rows, positions):
    gain_a, gain_b, w_query, w_key, w_value, w_out, w_gate, w_up, w_down = weights
    act_f = act_rows.astype(jnp.float32)
    normed_a = to_bf(act_f * rms_scale(act_f) * gain_a)
    q_rot = to_bf(rope_apply(jnp.einsum("sd,dhe->she", normed_a, w_query), positions))
    k_rot = to_bf(rope_apply(jnp.einsum("sd,dhe->she", normed_a, w_key), positions))
    v_proj = to_bf(jnp.einsum("sd,dhe->she", normed_a, w_value))
    q_groups = q_rot.reshape(N_BLOCKS, Q_BLOCK, KV_HEADS, N_GROUP, HEAD_DIM)
    block_starts = jnp.arange(N_BLOCKS) * Q_BLOCK
    key_index = jnp.arange(SEQ_LEN)

    def one_block(block_item):
        q_blk, q_start = block_item
        scores = jnp.einsum("qkgd,skd->kgqs", q_blk, k_rot) * ATTN_SCALE
        allowed = (q_start + jnp.arange(Q_BLOCK))[:, None] >= key_index[None, :]
        scores = jnp.where(allowed, scores, NEG_BIG)
        prob_rows = to_bf(jax.nn.softmax(scores, axis=-1))
        return to_bf(jnp.einsum("kgqs,skd->qkgd", prob_rows, v_proj))

    attn_rows = lax.map(jax.checkpoint(one_block), (q_groups, block_starts)).reshape(SEQ_LEN, Q_HEADS * HEAD_DIM)
    hidden = to_bf(act_f + jnp.dot(attn_rows, w_out))
    normed_b = to_bf(hidden * rms_scale(hidden) * gain_b)
    mixed_act = to_bf(jax.nn.silu(jnp.dot(normed_b, w_gate)) * jnp.dot(normed_b, w_up))
    return (hidden + jnp.dot(mixed_act, w_down)).astype(jnp.bfloat16)


def reference(act_in, positions, out_grad, norm1_gain, norm2_gain, w_query, w_key, w_value, w_out, w_gate, w_up, w_down):
    weights = tuple(param.astype(jnp.float32) for param in (norm1_gain, norm2_gain, w_query, w_key, w_value, w_out, w_gate, w_up, w_down))
    zero_grads = tuple(jnp.zeros_like(param) for param in weights)

    def per_sequence(grad_sums, seq_item):
        act_row, pos_row, grad_row = seq_item

        def fwd_fn(params, act_rows):
            return layer_forward(params, act_rows, pos_row)

        act_out, pullback = jax.vjp(fwd_fn, weights, act_row)
        param_grads, act_grad = pullback(grad_row)
        new_sums = tuple(run_sum + seq_grad for run_sum, seq_grad in zip(grad_sums, param_grads))
        return new_sums, (act_out, act_grad)

    grad_sums, outs = lax.scan(per_sequence, zero_grads, (act_in, positions, out_grad))
    return (outs[0], outs[1], grad_sums[0], grad_sums[1], grad_sums[2], grad_sums[3], grad_sums[4], grad_sums[5], grad_sums[6], grad_sums[7], grad_sums[8])
```

```python
import functools
import jax
import jax.numpy as jnp
from jax import lax
from jax.experimental import pallas as pl
from jax.experimental.pallas import tpu as pltpu
from jax.sharding import PartitionSpec as P

EPS = 1e-5
ROPE_BASE = 10000.0
NEG_BIG = -1e30
F32 = jnp.float32
BF16 = jnp.bfloat16


X_SWAP = ((0, 2), (2, 0), (1, 3), (3, 1))
C_SWAP = ((0, 1), (1, 0), (2, 3), (3, 2))
Y_SWAP = ((0, 1), (1, 0))


def swap_x(v):
    return lax.ppermute(v, "sp", X_SWAP)


def swap_c(v):
    return lax.ppermute(v, "sp", C_SWAP)


def swap_y(v):
    return lax.ppermute(v, "dp", Y_SWAP)


def pick(v, i, axis=0):
    return lax.dynamic_index_in_dim(v, i, axis, keepdims=False)


def rows_at(v, i, n):
    return lax.dynamic_slice_in_dim(v, i * n, n, 0)


def cols_at(v, i, n):
    return lax.dynamic_slice_in_dim(v, i * n, n, 1)


def put(buf, v, r, c):
    return lax.dynamic_update_slice(buf, v, (r, c))


def mm(a, b):
    return jnp.dot(a, b, preferred_element_type=F32)


def tie(v, *deps):
    return lax.optimization_barrier((v,) + deps)[0]


def dot_nt(a, b):
    return lax.dot_general(a, b, (((1,), (1,)), ((), ())), preferred_element_type=F32)


def dot_tn(a, b):
    return lax.dot_general(a, b, (((0,), (0,)), ((), ())), preferred_element_type=F32)


def rotate_halves(v, half):
    width = v.shape[-1]
    lane = lax.broadcasted_iota(jnp.int32, v.shape, 1)
    return jnp.where(lane % (2 * half) < half, pltpu.roll(v, width - half, 1), pltpu.roll(v, half, 1))


def attn_fwd_kernel(blk, dh, q_ref, k_ref, v_ref, o_ref, lse_ref):
    seq, width = q_ref.shape
    scale = dh ** -0.5
    keep = lax.broadcasted_iota(jnp.int32, (blk, blk), 0) <= lax.broadcasted_iota(jnp.int32, (blk, blk), 1)
    lse_ref[...] = jnp.zeros_like(lse_ref)
    for qi in range(seq // blk):
        rows = pl.ds(qi * blk, blk)
        outs = []
        for h in range(width // dh):
            cols = pl.ds(h * dh, dh)
            q = q_ref[rows, cols]
            s = []
            for j in range(qi + 1):
                st = dot_nt(k_ref[pl.ds(j * blk, blk), cols], q) * scale
                s.append(jnp.where(keep, st, NEG_BIG) if j == qi else st)
            top = s[0].max(0, keepdims=True)
            for t in s[1:]:
                top = jnp.maximum(top, t.max(0, keepdims=True))
            e = [jnp.exp(t - top) for t in s]
            tot = e[0].sum(0, keepdims=True)
            for t in e[1:]:
                tot = tot + t.sum(0, keepdims=True)
            inv = 1.0 / tot
            acc = None
            for j in range(qi + 1):
                p = (e[j] * inv).astype(BF16)
                part = dot_tn(v_ref[pl.ds(j * blk, blk), cols], p)
                acc = part if acc is None else acc + part
            outs.append(acc)
            lse_ref[0, pl.ds(h, 1), rows] = top + jnp.log(tot)
        o_ref[rows, :] = jnp.concatenate(outs, axis=0).T.astype(BF16)


def attn_bwd_kernel(blk, dh, q_ref, k_ref, v_ref, g_ref, lse_ref, cos_ref, sin_ref, dq_ref, dk_ref, dv_ref, dk_acc, dv_acc):
    seq, width = q_ref.shape
    scale = dh ** -0.5
    keep = lax.broadcasted_iota(jnp.int32, (blk, blk), 0) <= lax.broadcasted_iota(jnp.int32, (blk, blk), 1)

    def unrope(v, rows):
        v = v.astype(BF16).astype(F32)
        return (v * cos_ref[rows, :] - rotate_halves(v, dh // 2) * sin_ref[rows, :]).astype(BF16)

    for qi in range(seq // blk):
        rows = pl.ds(qi * blk, blk)
        dqs = []
        for h in range(width // dh):
            cols = pl.ds(h * dh, dh)
            q = q_ref[rows, cols]
            g = g_ref[rows, cols]
            lse = lse_ref[0, pl.ds(h, 1), rows]
            ps, dps = [], []
            delta = None
            for j in range(qi + 1):
                keys = pl.ds(j * blk, blk)
                st = dot_nt(k_ref[keys, cols], q) * scale
                p = jnp.exp(st - lse)
                if j == qi:
                    p = jnp.where(keep, p, 0.0)
                dp = dot_nt(v_ref[keys, cols], g)
                part = (p * dp).sum(0, keepdims=True)
                delta = part if delta is None else delta + part
                ps.append(p)
                dps.append(dp)
            dq = None
            for j in range(qi + 1):
                keys = pl.ds(j * blk, blk)
                ds = (ps[j] * (dps[j] - delta) * scale).astype(BF16)
                part = dot_tn(k_ref[keys, cols], ds)
                dq = part if dq is None else dq + part
                dk = jnp.dot(ds, q, preferred_element_type=F32)
                dv = jnp.dot(ps[j].astype(BF16), g, preferred_element_type=F32)
                if j == qi:
                    dk_acc[keys, cols] = dk
                    dv_acc[keys, cols] = dv
                else:
                    dk_acc[keys, cols] += dk
                    dv_acc[keys, cols] += dv
            dqs.append(dq)
        dq_ref[rows, :] = unrope(jnp.concatenate(dqs, axis=0).T, rows)
    for j in range(seq // blk):
        rows = pl.ds(j * blk, blk)
        dk_ref[rows, :] = unrope(dk_acc[rows, :], rows)
        dv_ref[rows, :] = dv_acc[rows, :].astype(BF16)


def qkv_kernel(dh, u_ref, w_ref, cos_ref, sin_ref, o_ref):
    width = w_ref.shape[0] // 3
    lanes = cos_ref.shape[1]
    for part in range(3):
        z = dot_nt(u_ref[...], w_ref[pl.ds(part * width, width), :])
        if part < 2:
            for c in range(0, width, lanes):
                zc = z[:, c:c + lanes]
                o_ref[:, pl.ds(part * width + c, lanes)] = (zc * cos_ref[...] + rotate_halves(zc, dh // 2) * sin_ref[...]).astype(BF16)
        else:
            o_ref[:, pl.ds(part * width, width)] = z.astype(BF16)


def qkv_project(u, w, cos_t, sin_t, dh):
    n_tok, dim = u.shape
    cols = w.shape[0]
    bt = 256
    return pl.pallas_call(
        functools.partial(qkv_kernel, dh), name="qkv_project",
        grid=(n_tok // bt,),
        in_specs=[pl.BlockSpec((bt, dim), lambda i: (i, 0)), pl.BlockSpec((cols, dim), lambda i: (0, 0)),
                  pl.BlockSpec((bt, 128), lambda i: (i, 0)), pl.BlockSpec((bt, 128), lambda i: (i, 0))],
        out_specs=pl.BlockSpec((bt, cols), lambda i: (i, 0)),
        out_shape=jax.ShapeDtypeStruct((n_tok, cols), BF16),
        cost_estimate=pl.CostEstimate(flops=2 * n_tok * dim * cols, bytes_accessed=2 * (n_tok * dim + cols * dim + n_tok * cols), transcendentals=0),
    )(u, w, cos_t, sin_t)


def attn_forward(qkv, seq, dh):
    n_tok, cols = qkv.shape
    width = cols // 3
    lanes = 128
    hp = width // lanes
    spec = lambda off: pl.BlockSpec((seq, lanes), lambda s, p, off=off: (s, off + p))
    return pl.pallas_call(
        functools.partial(attn_fwd_kernel, 256, dh), name="attn_fwd",
        grid=(n_tok // seq, hp),
        in_specs=[spec(0), spec(hp), spec(2 * hp)],
        out_specs=[pl.BlockSpec((seq, lanes), lambda s, p: (s, p)), pl.BlockSpec((1, 8, seq), lambda s, p: (s * hp + p, 0, 0))],
        out_shape=[jax.ShapeDtypeStruct((n_tok, width), BF16), jax.ShapeDtypeStruct((n_tok // seq * hp, 8, seq), F32)],
        cost_estimate=pl.CostEstimate(flops=16 * n_tok * seq * width // 4, bytes_accessed=8 * n_tok * width, transcendentals=n_tok * seq * width // dh // 2),
    )(qkv, qkv, qkv)


def attn_backward(qkv, grad_o, lse, cos_t, sin_t, seq, dh):
    n_tok, cols = qkv.shape
    width = cols // 3
    lanes = 128
    hp = width // lanes
    spec = lambda off: pl.BlockSpec((seq, lanes), lambda s, p, off=off: (s, off + p))
    tab = pl.BlockSpec((seq, lanes), lambda s, p: (s, 0))
    return pl.pallas_call(
        functools.partial(attn_bwd_kernel, 256, dh), name="attn_bwd",
        grid=(n_tok // seq, hp),
        in_specs=[spec(0), spec(hp), spec(2 * hp), spec(0), pl.BlockSpec((1, 8, seq), lambda s, p: (s * hp + p, 0, 0)), tab, tab],
        out_specs=[spec(0)] * 3,
        out_shape=[jax.ShapeDtypeStruct((n_tok, width), BF16)] * 3,
        scratch_shapes=[pltpu.VMEM((seq, lanes), F32), pltpu.VMEM((seq, lanes), F32)],
        cost_estimate=pl.CostEstimate(flops=40 * n_tok * seq * width // 4, bytes_accessed=16 * n_tok * width, transcendentals=n_tok * seq * width // dh // 2),
    )(qkv, qkv, qkv, grad_o, lse, cos_t, sin_t)


def rms_forward(rows_f32, gain_f32):
    row_scale = lax.rsqrt(jnp.mean(rows_f32 * rows_f32, axis=-1, keepdims=True) + EPS)
    unit_rows = rows_f32 * row_scale
    return (unit_rows * gain_f32).astype(BF16), unit_rows, row_scale


def rms_backward(grad_normed, unit_rows, row_scale, gain_f32):
    gain_grad = jnp.sum(grad_normed * unit_rows, axis=0)
    grad_unit = grad_normed * gain_f32
    inner_mean = jnp.mean(grad_unit * unit_rows, axis=-1, keepdims=True)
    return row_scale * (grad_unit - unit_rows * inner_mean), gain_grad


def to_inner(v):
    n = v.shape[-1] // 8
    return jnp.concatenate([v[..., (4 * y + s) * n:(4 * y + s + 1) * n] for s in range(4) for y in range(2)], axis=-1)


def to_outer(v):
    n = v.shape[-1] // 8
    return jnp.concatenate([v[..., (2 * s + y) * n:(2 * s + y + 1) * n] for y in range(2) for s in range(4)], axis=-1)


def solution(mesh):
    flat_axes = ("dp", "sp")
    row_spec = P("dp", "sp", None)
    pos_spec = P("dp", "sp")
    vec_spec = P(flat_axes)
    mat_spec = P(flat_axes, None)
    cube_spec = P(flat_axes, None, None)

    def gather(local_part):
        return lax.all_gather(local_part, flat_axes, axis=0, tiled=True)

    def local_step(act_in, positions, out_grad, norm1_gain, norm2_gain, w_query, w_key, w_value, w_out, w_gate, w_up, w_down):
        iy = lax.axis_index("dp")
        isp = lax.axis_index("sp")
        ix = isp >> 1
        ic = isp & 1
        oy, ox, oc = 1 - iy, 1 - ix, 1 - ic
        tok, dim = act_in.shape[1], act_in.shape[2]
        n_tok = tok * 8
        n_heads, dh = w_query.shape[1], w_query.shape[2]
        hcol = n_heads // 8 * dh
        ffn = w_gate.shape[1]
        fcol = ffn // 8
        drow = dim // 8
        x_rows = act_in[0]
        dy = out_grad[0]
        blks = (2 * ix + ic, 2 * ix + oc, 2 * ox + ic, 2 * ox + oc)

        small = jnp.stack([norm1_gain.astype(F32), norm2_gain.astype(F32), positions[0].astype(F32)])
        small_full = lax.all_gather(small, flat_axes, axis=0, tiled=False)
        gain1 = small_full[:, 0].reshape(dim)
        gain2 = small_full[:, 1].reshape(dim)
        pos_full = small_full[:, 2].reshape(n_tok)
        gain1_in = to_inner(gain1)
        gain2_in = to_inner(gain2)

        def gather_qkv(w):
            wt = w.transpose(1, 2, 0).reshape(n_heads * dh, drow)
            n = n_heads * dh // 2
            got = swap_y(rows_at(wt, oy, n))
            wb = jnp.zeros((n, 2 * drow), BF16)
            wb = put(wb, rows_at(wt, iy, n), 0, iy * drow)
            wb = put(wb, got, 0, oy * drow)
            got_x = swap_x(rows_at(wb, ox, 2 * hcol))
            send_c = jnp.concatenate([rows_at(wb, blks[1], hcol), rows_at(got_x, oc, hcol)], axis=1)
            got_c = swap_c(send_c)
            fin = jnp.zeros((hcol, dim), BF16)
            fin = put(fin, rows_at(wb, blks[0], hcol), 0, blks[0] * 2 * drow)
            fin = put(fin, rows_at(got_x, ic, hcol), 0, blks[2] * 2 * drow)
            fin = put(fin, got_c[:, :2 * drow], 0, blks[1] * 2 * drow)
            fin = put(fin, got_c[:, 2 * drow:], 0, blks[3] * 2 * drow)
            return wb, fin

        def gather_ffn(w):
            got = swap_y(cols_at(w, oy, ffn // 2))
            wb = jnp.zeros((2 * drow, ffn // 2), BF16)
            wb = put(wb, cols_at(w, iy, ffn // 2), iy * drow, 0)
            wb = put(wb, got, oy * drow, 0)
            got_x = swap_x(cols_at(wb, ox, 2 * fcol))
            send_c = jnp.concatenate([cols_at(wb, blks[1], fcol), cols_at(got_x, oc, fcol)], axis=0)
            got_c = swap_c(send_c)
            fin = jnp.zeros((dim, fcol), BF16)
            fin = put(fin, cols_at(wb, blks[0], fcol), blks[0] * 2 * drow, 0)
            fin = put(fin, cols_at(got_x, ic, fcol), blks[2] * 2 * drow, 0)
            fin = put(fin, got_c[:2 * drow], blks[1] * 2 * drow, 0)
            fin = put(fin, got_c[2 * drow:], blks[3] * 2 * drow, 0)
            return wb, fin

        wbq, wfq = gather_qkv(w_query)
        wbk, wfk = gather_qkv(w_key)
        wbv, wfv = gather_qkv(w_value)
        w_qkv = jnp.concatenate([wfq, wfk, wfv], axis=0)
        act_f = x_rows.astype(F32)
        normed_a, unit_a, scale_a = rms_forward(act_f, gain1)
        u_full = gather(to_inner(normed_a))

        half = dh // 2
        inv_freq = ROPE_BASE ** (-(jnp.arange(half, dtype=F32) * (2.0 / dh)))
        angles = pos_full[:, None] * inv_freq
        cos_h, sin_h = jnp.cos(angles), jnp.sin(angles)
        cos_t = jnp.concatenate([cos_h] * 4, axis=1)
        sin_t = jnp.concatenate([-sin_h, sin_h] * 2, axis=1)

        qkv = qkv_project(u_full, w_qkv, cos_t, sin_t, dh)
        attn_o, lse = attn_forward(qkv, n_tok // 2, dh)

        wo_full = gather(w_out)
        o_tok = lax.all_to_all(attn_o.reshape(8, tok, hcol), flat_axes, 0, 0, tiled=True)
        o_tok = o_tok.transpose(1, 0, 2).reshape(tok, dim)
        hidden = (act_f + mm(o_tok, wo_full)).astype(BF16)
        hidden_f = hidden.astype(F32)
        normed_b, unit_b, scale_b = rms_forward(hidden_f, gain2)
        w_full = gather(to_inner(normed_b))
        wb1, wf1 = gather_ffn(w_gate)
        wb3, wf3 = gather_ffn(w_up)
        gate_pre = mm(w_full, wf1)
        up_pre = mm(w_full, wf3)
        gate_sig = jax.nn.sigmoid(gate_pre)
        gate_act = gate_pre * gate_sig
        mixed = (gate_act * up_pre).astype(BF16)

        w2_got = swap_c(w_down)
        m5 = mixed.reshape(2, 2, 2, tok, fcol)
        m_own = pick(m5, ic, 2)
        m_got = swap_c(pick(m5, oc, 2))
        hd = dim // 2

        def part(axis, i, lo):
            a = pick(m_own, i, axis).reshape(2 * tok, fcol)
            b = pick(m_got, i, axis).reshape(2 * tok, fcol)
            return mm(a, w_down[:, lo:lo + hd]) + mm(b, w2_got[:, lo:lo + hd])

        ga = swap_x(part(1, ox, 0))
        gb = swap_y(part(0, oy, hd))
        ta = part(1, ix, 0) + ga
        tb = part(0, iy, hd) + gb
        fa = rows_at(ta, iy, tok) + swap_y(rows_at(ta, oy, tok))
        fb = rows_at(tb, ix, tok) + swap_x(rows_at(tb, ox, tok))
        act_out = (hidden_f + jnp.concatenate([fa, fb], axis=1)).astype(BF16)

        dy_full = gather(dy)
        grad_mixed = dot_nt(dy_full, w_down).astype(BF16).astype(F32)
        down_grad = dot_tn(mixed, dy_full)
        grad_up = (grad_mixed * gate_act).astype(BF16)
        grad_gate = (grad_mixed * up_pre * gate_sig * (1.0 + gate_pre * (1.0 - gate_sig))).astype(BF16)

        def pieces(v):
            vx = swap_x(v)
            return (v, swap_c(v), vx, swap_c(vx))

        w_sl = cols_at(w_full, isp, 2 * drow)
        w_sl_t = w_sl.T
        w_send, w_keep = rows_at(w_sl_t, oy, drow), rows_at(w_sl_t, iy, drow)

        def ffn_back(g, wb):
            out = jnp.zeros((drow, ffn), F32)
            total = None
            for blk, piece in zip(blks, pieces(g)):
                sent = swap_y(mm(w_send, piece))
                p = dot_nt(piece, cols_at(wb, blk, fcol))
                total = p if total is None else total + p
                out = put(out, mm(w_keep, piece), 0, (iy * 4 + blk) * fcol)
                out = put(out, sent, 0, (oy * 4 + blk) * fcol)
            return total, out

        dw_g, gate_grad = ffn_back(grad_gate, wb1)
        dw_u, up_grad = ffn_back(grad_up, wb3)

        def to_rows(p):
            tot = (rows_at(p, iy, n_tok // 2) + swap_y(rows_at(p, oy, n_tok // 2))).astype(BF16)
            tot = tot.reshape(2, 2, tok, 2 * drow)
            own = pick(tot, ic, 1)
            got = swap_c(pick(tot, oc, 1))
            got_x = swap_x(jnp.concatenate([pick(own, ox), pick(got, ox)], axis=1))
            res = jnp.zeros((tok, dim), BF16)
            w = 2 * drow
            for blk, v in zip(blks, (pick(own, ix), pick(got, ix), got_x[:, :w], got_x[:, w:])):
                res = put(res, v, 0, blk * w)
            return to_outer(res)

        grad_normed_b = to_rows(dw_g + dw_u).astype(F32)
        grad_rows_b, gain2_grad = rms_backward(grad_normed_b, unit_b, scale_b, gain2)
        grad_hidden = (dy.astype(F32) + grad_rows_b).astype(BF16)
        dh_full = gather(grad_hidden)
        grad_attn = dot_nt(dh_full, w_out).astype(BF16)
        wout_grad = dot_tn(attn_o, dh_full)
        gq, gk, gv = attn_backward(qkv, grad_attn, lse, cos_t, sin_t, n_tok // 2, dh)

        u_sl = cols_at(u_full, isp, 2 * drow)
        u_send, u_keep = cols_at(u_sl, oy, drow), cols_at(u_sl, iy, drow)

        def qkv_back(g, wb):
            out = jnp.zeros((n_heads * dh, drow), F32)
            total = None
            for blk, piece in zip(blks, pieces(g)):
                sent = swap_y(dot_tn(piece, u_send))
                p = mm(piece, rows_at(wb, blk, hcol))
                total = p if total is None else total + p
                out = put(out, dot_tn(piece, u_keep), (iy * 4 + blk) * hcol, 0)
                out = put(out, sent, (oy * 4 + blk) * hcol, 0)
            return total, out.reshape(n_heads, dh, drow).transpose(2, 0, 1)

        du_q, query_grad = qkv_back(gq, wbq)
        du_k, key_grad = qkv_back(gk, wbk)
        du_v, value_grad = qkv_back(gv, wbv)
        grad_normed_a = to_rows(du_q + du_k + du_v).astype(F32)
        grad_rows_a, gain1_grad = rms_backward(grad_normed_a, unit_a, scale_a, gain1)
        in_grad = (grad_hidden.astype(F32) + grad_rows_a).astype(BF16)
        gains = jnp.stack([gain1_grad.reshape(8, drow), gain2_grad.reshape(8, drow)], axis=1)
        gains = lax.psum(gains, flat_axes)
        gains = pick(gains, iy * 4 + isp)
        return (act_out[None], in_grad[None], gains[0], gains[1], query_grad, key_grad, value_grad, wout_grad, gate_grad, up_grad, down_grad)

    return jax.shard_map(local_step, mesh=mesh, in_specs=(row_spec, pos_spec, row_spec, vec_spec, vec_spec, cube_spec, cube_spec, cube_spec, mat_spec, mat_spec, mat_spec, mat_spec), out_specs=(row_spec, row_spec, vec_spec, vec_spec, cube_spec, cube_spec, cube_spec, mat_spec, mat_spec, mat_spec, mat_spec), check_vma=False)
```
